256 devices in a mesh: blk: 64 (over y, x, z_lo, core), tp: 4 (over z_hi).
Axes of the slice: x: 4, y: 4, z: 8 (z_hi: 4, z_lo: 2; z = z_hi * 2 + z_lo), core: 2. Of those that a mesh axis runs over, the one named last changes fastest.
Arguments:
- queries: bfloat16 [16384, 32, 128], P(('blk', 'tp')), may hold values from -100 to 100
- keys: bfloat16 [16384, 4, 128], P(('blk', 'tp')), may hold values from -6 to 6
- values: bfloat16 [16384, 4, 128], P(('blk', 'tp')), may hold values from -6 to 6
- span_order: int32 [128], replicated, may hold values from 0 to 127, each once
- doc_ids: int32 [16384], replicated, may hold values from 0 to 31, never falling along the last dimension, each value on 1 to 2048 neighbouring positions
Outputs:
- attended: bfloat16 [16384, 32, 128], P(('blk', 'tp'))
The draws below stay inside these ranges and needn't reach their ends.
Inputs may be any that keep to these rules, and one draw needn't show every extreme that they name: `span_order`: each span number appears exactly once. `doc_ids`: document numbers never fall along the sequence; each document has at most 2048 tokens and one has exactly that many.
All inputs are finite; a program needn't handle non-finite values.
Results may differ from the reference program's by a relative error of at most 0.004.
Values may be sent and summed in bfloat16 or wider, within the bound.
No kernel may reach another device: no remote copies, remote signals or barrier semaphores. Data moves between devices by JAX's collectives and lax.ppermute only.
A program may use at most 64 MiB of HBM per device.

```python
import math
import jax
import jax.numpy as jnp
import numpy as np
from jax import lax

QUERY_HEADS = 32
KEY_VALUE_HEADS = 4
HEAD_SIZE = 128
SPAN = 128
DOCS = 32
SEQUENCE_TOKENS = 16384
N_BLK = 64


def draw_pair(key):
    base = jax.random.fold_in(key, 29)
    key_q, key_slice = jax.random.split(base, 2)
    keys_float = jax.random.normal(key_slice, (SEQUENCE_TOKENS, KEY_VALUE_HEADS, HEAD_SIZE), jnp.float32)
    queries_f = jax.random.normal(key_q, (SEQUENCE_TOKENS, QUERY_HEADS, HEAD_SIZE), jnp.float32)
    return (queries_f, keys_float)


def draw_queries(key, part):
    return jnp.clip(draw_pair(key)[0], -100.0, 100.0).astype(jnp.bfloat16)


def draw_keys(key, part):
    return jnp.clip(draw_pair(key)[1], -6.0, 6.0).astype(jnp.bfloat16)


def shard_levels(key, shape, shards, least, top_value):
    gain, own = 1.0, jax.random.fold_in(key, 6)
    for dim, blocks in shards:
        heights = jnp.exp(jax.random.uniform(jax.random.fold_in(own, dim), (blocks,), jnp.float32, least / len(shards), top_value / len(shards)))
        gain = gain * jnp.repeat(heights, shape[dim] // blocks).reshape([-1 if axis == dim else 1 for axis in range(len(shape))])
    return gain


def length_profile(amount, total, most, lean):
    loads = [(1 << 20) // math.isqrt(rank ** lean) + 1 for rank in range(2, amount + 1)]
    surplus, holding = total - most - (amount - 1), [1] * (amount - 1)
    while surplus > 0:
        movable = [i for i in range(amount - 1) if holding[i] < most]
        whole, remaining = sum([loads[i] for i in movable]), surplus
        for i in movable:
            extra = min(most - holding[i], max(1, remaining * loads[i] // whole), surplus)
            holding[i] = holding[i] + extra
            surplus = surplus - extra
    return np.array([most] + holding)


def uneven_parts(key, number_of, total, limit, skew):
    if number_of == 2:
        one = jax.random.randint(key, (), max(1, total - limit), min(limit, total - 1) + 1)
        return jnp.stack([one, total - one])
    lengths = jnp.asarray(length_profile(number_of, total, limit, skew), jnp.int32)
    couples = (number_of - 1) // 2
    source_of, taker = lengths[1:1 + 2 * couples:2], lengths[2:2 + 2 * couples:2]
    slack = jnp.minimum(source_of - 1, limit - taker)
    passed = jax.random.randint(jax.random.fold_in(key, 1), (couples,), 0, 1 << 20) % (slack + 1)
    lengths = lengths.at[1:1 + 2 * couples:2].set(source_of - passed).at[2:2 + 2 * couples:2].set(taker + passed)
    return lengths[jax.random.permutation(jax.random.fold_in(key, 2), number_of)]


def noise(stream_key, extent, width, bound, shards=(), kind=jnp.bfloat16):
    factor_of = shard_levels(stream_key, extent, shards, -0.22, 0.18) if shards else 1.0
    entries = jax.random.normal(stream_key, extent, jnp.float32) * width * factor_of
    return jnp.minimum(jnp.maximum(entries, -bound), bound).astype(kind)


def setup_inputs(seed: int = 0) -> dict:
    arg_keys = jax.random.split(jax.random.key(seed), 6)
    return {
        "queries": draw_queries(jax.random.fold_in(arg_keys[5], 71), 0),
        "keys": draw_keys(jax.random.fold_in(arg_keys[5], 71), 0),
        "values": noise(arg_keys[2], (SEQUENCE_TOKENS, KEY_VALUE_HEADS, HEAD_SIZE), 1.0, 6.0, ((0, 256),)),
        "span_order": jax.random.permutation(arg_keys[3], 2 * N_BLK).astype(jnp.int32),
        "doc_ids": jnp.searchsorted(jnp.cumsum(uneven_parts(arg_keys[4], DOCS, SEQUENCE_TOKENS, SEQUENCE_TOKENS // 8, 0)), jnp.arange(SEQUENCE_TOKENS), side="right").astype(jnp.int32),
    }


def reference(queries, keys, values, span_order, doc_ids):
    rows = jnp.arange(SEQUENCE_TOKENS, dtype=jnp.int32)
    pos = (span_order[rows // SPAN] * SPAN + rows % SPAN).astype(jnp.int32)
    docs = doc_ids[pos]
    group_size = QUERY_HEADS // KEY_VALUE_HEADS
    scale = 1.0 / math.sqrt(HEAD_SIZE)
    block_tile = math.gcd(SEQUENCE_TOKENS, 64)
    key_all = keys.astype(jnp.float32)
    value_all = values.astype(jnp.float32)
    query_block_list = queries.reshape(SEQUENCE_TOKENS // block_tile, block_tile, KEY_VALUE_HEADS, group_size, HEAD_SIZE)
    pos_blocks = pos.reshape(SEQUENCE_TOKENS // block_tile, block_tile)
    doc_blocks = docs.reshape(SEQUENCE_TOKENS // block_tile, block_tile)

    def one_block(item):
        query_part, query_pos, query_doc = item
        scores = jnp.einsum('qhgd,khd->hgqk', query_part.astype(jnp.float32), key_all) * scale
        allowed = (pos[None, :] <= query_pos[:, None]) & (docs[None, :] == query_doc[:, None])
        scores = jnp.where(allowed, scores, -1e+30)
        top = lax.optimization_barrier(jnp.max(scores, axis=-1))
        expo = jnp.where(allowed, jnp.exp(scores - top[..., None]), 0.0)
        total = lax.optimization_barrier(jnp.sum(expo, axis=-1))
        weights = lax.optimization_barrier(expo.astype(jnp.bfloat16)).astype(jnp.float32)
        summed = jnp.einsum('hgqk,khd->hgqd', weights, value_all)
        result = summed / total[..., None]
        return jnp.transpose(result, (2, 0, 1, 3)).reshape(block_tile, QUERY_HEADS, HEAD_SIZE).astype(jnp.bfloat16)
    outputs = lax.map(one_block, (query_block_list, pos_blocks, doc_blocks))
    return outputs.reshape(SEQUENCE_TOKENS, QUERY_HEADS, HEAD_SIZE)
```

```python
import math

import jax
import jax.numpy as jnp
from jax import lax
from jax.experimental import pallas as pl
from jax.experimental.pallas import tpu as pltpu
from jax.sharding import Mesh, PartitionSpec as P

SPAN = 128
BACK = 16
DOCS = 32
ALL = ("y", "x", "z", "c", "tp")
PLANE = ("c", "y", "x")
NEG = -1e30


def pieces_kernel(me_ref, q_ref, kv_ref, p0, p1, p2, p3, sems):
    me = me_ref[0]
    copies = []
    for k, out in enumerate((p0, p1, p2, p3)):
        head = lax.rem(me + k, 4)
        copies.append(pltpu.make_async_copy(q_ref.at[:, head], out.at[pl.ds(0, 64)], sems.at[2 * k]))
        copies.append(pltpu.make_async_copy(kv_ref.at[head], out.at[pl.ds(64, 16)], sems.at[2 * k + 1]))
    for copy in copies:
        copy.start()
    for copy in copies:
        copy.wait()


def windows_kernel(order_ref, z_ref, spread_ref, out_ref, ordered, sems):
    z = z_ref[0]
    ordered[pl.ds(0, BACK)] = jnp.zeros((BACK, 8, SPAN), jnp.bfloat16)

    def place(slot, _):
        ordered[order_ref[slot] + BACK] = spread_ref[slot]
        return 0

    lax.fori_loop(0, 128, place, 0, unroll=8)
    copies = []
    for dest in range(32):
        block = (dest % 16) * 4 + z * 2 + dest // 16
        for slot in range(2):
            span = order_ref[2 * block + slot]
            copies.append(
                pltpu.make_async_copy(
                    ordered.at[pl.ds(span, BACK)], out_ref.at[dest, slot], sems.at[2 * dest + slot]
                )
            )
    for copy in copies:
        copy.start()
    for copy in copies:
        copy.wait()


def attention_kernel(me_ref, reach_ref, first_ref, kv_ref, p0, p1, p2, p3, out_ref, own, sems):
    me = me_ref[0]
    copies = []
    for k, piece in enumerate((p0, p1, p2, p3)):
        copies.append(pltpu.make_async_copy(piece, own.at[lax.rem(me + 4 - k, 4)], sems.at[k]))
    for copy in copies:
        copy.start()
    for copy in copies:
        copy.wait()
    factor = math.log2(math.e) / math.sqrt(SPAN)
    rows = 256

    def slot_pass(slot, spans):
        width = 16 * 8 * spans
        lane = lax.broadcasted_iota(jnp.int32, (1, width), 1)
        chunk, inner = lane // (8 * spans), lane % (8 * spans)
        span, r = inner // 8 + (BACK - spans), inner % 8
        rel = span * SPAN + (r // 4) * 64 + chunk * 4 + r % 4
        keys = kv_ref[0:16, slot, BACK - spans : BACK].reshape(width, SPAN)
        values = kv_ref[16:32, slot, BACK - spans : BACK].reshape(width, SPAN)
        own_keys = jnp.concatenate([own[2 * slot + h, 64:72].reshape(64, SPAN) for h in range(2)], axis=0)
        own_values = jnp.concatenate([own[2 * slot + h, 72:80].reshape(64, SPAN) for h in range(2)], axis=0)
        own_rel = lax.broadcasted_iota(jnp.int32, (1, SPAN), 1) + BACK * SPAN
        for part in range(1024 // rows):
            half, at = part // 2, (part % 2) * (rows // 8)
            query = own[2 * slot + half, at : at + rows // 8].reshape(rows, SPAN)
            first = first_ref[pl.ds(slot * 1024 + part * rows, rows)]
            mine = (
                lax.broadcasted_iota(jnp.int32, (rows, 1), 0) // 8 + (part * rows // 8 + BACK * SPAN)
            )
            contract = (((1,), (1,)), ((), ()))
            far = lax.dot_general(query, keys, contract, preferred_element_type=jnp.float32)
            near = lax.dot_general(query, own_keys, contract, preferred_element_type=jnp.float32)
            far = jnp.where(rel >= first, far, NEG)
            near = jnp.where((own_rel >= first) & (own_rel <= mine), near, NEG)
            top = jnp.maximum(jnp.max(far, axis=1, keepdims=True), jnp.max(near, axis=1, keepdims=True))
            far = jnp.exp2((far - top) * factor)
            near = jnp.exp2((near - top) * factor)
            total = jnp.sum(far, axis=1, keepdims=True) + jnp.sum(near, axis=1, keepdims=True)
            summed = jnp.dot(far.astype(jnp.bfloat16), values, preferred_element_type=jnp.float32)
            summed += jnp.dot(near.astype(jnp.bfloat16), own_values, preferred_element_type=jnp.float32)
            to = lax.rem(2 * slot + half + 4 - me, 4)
            out_ref[to, at : at + rows // 8] = (
                (summed / total).astype(jnp.bfloat16).reshape(rows // 8, 8, SPAN)
            )

    for slot in range(2):
        reach = reach_ref[slot]
        sizes = (2, 4, 8, BACK)
        for low, high in zip((-1,) + sizes[:-1], sizes):

            @pl.when((reach > low) & (reach <= high))
            def _(slot=slot, high=high):
                slot_pass(slot, high)


def gather_kernel(me_ref, r0, r1, r2, r3, out_ref, sems):
    me = me_ref[0]
    copies = []
    for k, piece in enumerate((r0, r1, r2, r3)):
        copies.append(
            pltpu.make_async_copy(piece, out_ref.at[:, lax.rem(me + 4 - k, 4)], sems.at[k])
        )
    for copy in copies:
        copy.start()
    for copy in copies:
        copy.wait()


SMEM = pl.BlockSpec(memory_space=pltpu.SMEM)
ANY = pl.BlockSpec(memory_space=pl.ANY)
VMEM = pl.BlockSpec(memory_space=pltpu.VMEM)


def shifted(piece, by):
    return lax.ppermute(piece, "tp", [(i, (i + by) % 4) for i in range(4)])


def on_device(queries, keys, values, span_order, doc_ids):
    bf16 = jnp.bfloat16
    me = lax.axis_index("tp").astype(jnp.int32)
    z = lax.axis_index("z").astype(jnp.int32)
    block = lax.axis_index(ALL[:-1]).astype(jnp.int32)
    me1, z1 = me.reshape(1), z.reshape(1)

    by_head = jnp.concatenate([keys.transpose(1, 0, 2), values.transpose(1, 0, 2)], axis=1)
    sent = by_head.reshape(4, 2, 16, 4, SPAN).transpose(2, 1, 0, 3, 4)
    sent = jnp.broadcast_to(sent[:, None], (16, 2, 2, 4, 4, SPAN)).reshape(256, 4, SPAN)
    spread = lax.all_to_all(sent, ALL, 0, 0, tiled=True).reshape(128, 8, SPAN)

    pieces = pl.pallas_call(
        pieces_kernel,
        out_shape=[jax.ShapeDtypeStruct((80, 8, SPAN), bf16)] * 4,
        in_specs=[SMEM, ANY, ANY],
        out_specs=[ANY] * 4,
        scratch_shapes=[pltpu.SemaphoreType.DMA((8,))],
        name="pieces",
    )(me1, queries.reshape(64, 4, 8, SPAN), by_head.reshape(4, 16, 8, SPAN))
    pieces = [pieces[0]] + [shifted(pieces[k], k) for k in range(1, 4)]

    windows = pl.pallas_call(
        windows_kernel,
        out_shape=jax.ShapeDtypeStruct((32, 2, BACK, 8, SPAN), bf16),
        in_specs=[SMEM, SMEM, VMEM],
        out_specs=ANY,
        scratch_shapes=[pltpu.VMEM((128 + BACK, 8, SPAN), bf16), pltpu.SemaphoreType.DMA((64,))],
        name="windows",
    )(span_order, z1, spread)
    windows = lax.all_to_all(windows.reshape(32, 256, SPAN), PLANE, 0, 0, tiled=True)

    doc_first = jnp.sum(
        (doc_ids[None, :] < jnp.arange(DOCS, dtype=jnp.int32)[:, None]).astype(jnp.int32), axis=1
    )
    spans = lax.dynamic_slice_in_dim(span_order, 2 * block, 2)
    docs = jnp.stack([lax.dynamic_slice_in_dim(doc_ids, spans[i] * SPAN, SPAN) for i in range(2)])
    start = jnp.sum(
        jnp.where(docs[:, :, None] == jnp.arange(DOCS, dtype=jnp.int32), doc_first, 0), axis=-1
    )
    first = start - (spans[:, None] - BACK) * SPAN
    reach = jnp.clip(BACK - first[:, 0] // SPAN, 0, BACK)
    first = jnp.broadcast_to(first.reshape(256, 1), (256, 8)).reshape(2048, 1)

    attended = pl.pallas_call(
        attention_kernel,
        out_shape=jax.ShapeDtypeStruct((4, 64, 8, SPAN), bf16),
        in_specs=[SMEM, SMEM, VMEM, VMEM] + [ANY] * 4,
        out_specs=VMEM,
        scratch_shapes=[pltpu.VMEM((4, 80, 8, SPAN), bf16), pltpu.SemaphoreType.DMA((4,))],
        name="attention",
    )(me1, reach, first, windows.reshape(32, 2, BACK, 8, SPAN), *pieces)

    back = [attended[0]] + [shifted(attended[k], k) for k in range(1, 4)]
    result = pl.pallas_call(
        gather_kernel,
        out_shape=jax.ShapeDtypeStruct((64, 4, 8, SPAN), bf16),
        in_specs=[SMEM] + [ANY] * 4,
        out_specs=ANY,
        scratch_shapes=[pltpu.SemaphoreType.DMA((4,))],
        name="gather",
    )(me1, *back)
    return result.reshape(64, 32, SPAN)


def solution(mesh):
    fine = Mesh(mesh.devices.reshape(4, 4, 2, 2, 4), ALL)
    placed = (P(ALL, None, None), P(ALL, None, None), P(ALL, None, None), P(), P())
    return jax.shard_map(
        on_device, mesh=fine, in_specs=placed, out_specs=P(ALL, None, None), check_vma=False
    )
```

```python
import math

import jax
import jax.numpy as jnp
from jax import lax
from jax.experimental import pallas as pl
from jax.experimental.pallas import tpu as pltpu
from jax.sharding import Mesh, PartitionSpec as P

SPAN = 128
BACK = 16
DOCS = 32
ALL = ("y", "x", "z", "c", "tp")
PLANE = ("c", "y", "x")
NEG = -1e30


def pieces_kernel(me_ref, q_ref, kv_ref, p0, p1, p2, p3):
    me = me_ref[0]
    for k, out in enumerate((p0, p1, p2, p3)):
        head = lax.rem(me + k, 4)
        out[0:64] = q_ref[:, head]
        out[64:80] = kv_ref[head]


def windows_kernel(order_ref, z_ref, spread_ref, out_ref, ordered, sems):
    z = z_ref[0]
    ordered[pl.ds(0, BACK)] = jnp.zeros((BACK, 8, SPAN), jnp.bfloat16)

    def place(slot, _):
        ordered[order_ref[slot] + BACK] = spread_ref[slot]
        return 0

    lax.fori_loop(0, 128, place, 0, unroll=8)
    copies = []
    for dest in range(32):
        block = (dest % 16) * 4 + z * 2 + dest // 16
        for slot in range(2):
            span = order_ref[2 * block + slot]
            copies.append(
                pltpu.make_async_copy(
                    ordered.at[pl.ds(span, BACK)], out_ref.at[dest, slot], sems.at[2 * dest + slot]
                )
            )
    for copy in copies:
        copy.start()
    for copy in copies:
        copy.wait()


def attention_kernel(me_ref, reach_ref, first_ref, kv_ref, p0, p1, p2, p3, o0, o1, o2, o3, own, out):
    me = me_ref[0]
    for k, piece in enumerate((p0, p1, p2, p3)):
        own[lax.rem(me + 4 - k, 4)] = piece[...]
    factor = math.log2(math.e) / math.sqrt(SPAN)

    def slot_pass(slot, spans):
        rows = 512 if spans <= 8 else 256
        width = 16 * 8 * spans
        lane = lax.broadcasted_iota(jnp.int32, (1, width), 1)
        chunk, inner = lane // (8 * spans), lane % (8 * spans)
        span, r = inner // 8 + (BACK - spans), inner % 8
        rel = span * SPAN + (r // 4) * 64 + chunk * 4 + r % 4
        keys = kv_ref[0:16, slot, BACK - spans : BACK].reshape(width, SPAN)
        values = kv_ref[16:32, slot, BACK - spans : BACK].reshape(width, SPAN)
        own_keys = jnp.concatenate([own[2 * slot + h, 64:72].reshape(64, SPAN) for h in range(2)], axis=0)
        own_values = jnp.concatenate([own[2 * slot + h, 72:80].reshape(64, SPAN) for h in range(2)], axis=0)
        own_rel = lax.broadcasted_iota(jnp.int32, (1, SPAN), 1) + BACK * SPAN
        for part in range(1024 // rows):
            half, at = part * rows // 512, part * rows % 512 // 8
            query = own[2 * slot + half, at : at + rows // 8].reshape(rows, SPAN)
            first = first_ref[pl.ds(slot * 1024 + part * rows, rows)]
            mine = (
                lax.broadcasted_iota(jnp.int32, (rows, 1), 0) // 8 + (part * rows // 8 + BACK * SPAN)
            )
            contract = (((1,), (1,)), ((), ()))
            far = lax.dot_general(query, keys, contract, preferred_element_type=jnp.float32)
            near = lax.dot_general(query, own_keys, contract, preferred_element_type=jnp.float32)
            far = jnp.where(rel >= first, far, NEG)
            near = jnp.where((own_rel >= first) & (own_rel <= mine), near, NEG)
            top = jnp.maximum(jnp.max(far, axis=1, keepdims=True), jnp.max(near, axis=1, keepdims=True))
            far = jnp.exp2((far - top) * factor)
            near = jnp.exp2((near - top) * factor)
            total = jnp.sum(far, axis=1, keepdims=True) + jnp.sum(near, axis=1, keepdims=True)
            summed = jnp.dot(far.astype(jnp.bfloat16), values, preferred_element_type=jnp.float32)
            summed += jnp.dot(near.astype(jnp.bfloat16), own_values, preferred_element_type=jnp.float32)
            to = lax.rem(2 * slot + half + 4 - me, 4)
            out[to, at : at + rows // 8] = (
                (summed / total).astype(jnp.bfloat16).reshape(rows // 8, 8, SPAN)
            )

    for slot in range(2):
        reach = reach_ref[slot]
        sizes = (2, 4, 8, BACK)
        for low, high in zip((-1,) + sizes[:-1], sizes):

            @pl.when((reach > low) & (reach <= high))
            def _(slot=slot, high=high):
                slot_pass(slot, high)

    for k, piece in enumerate((o0, o1, o2, o3)):
        piece[...] = out[k]


def gather_kernel(me_ref, r0, r1, r2, r3, out_ref):
    me = me_ref[0]
    for k, piece in enumerate((r0, r1, r2, r3)):
        out_ref[:, lax.rem(me + 4 - k, 4)] = piece[...]


SMEM = pl.BlockSpec(memory_space=pltpu.SMEM)
ANY = pl.BlockSpec(memory_space=pl.ANY)
VMEM = pl.BlockSpec(memory_space=pltpu.VMEM)


def near(array):
    return pltpu.with_memory_space_constraint(array, pltpu.VMEM)


def shifted(piece, by):
    return lax.ppermute(piece, "tp", [(i, (i + by) % 4) for i in range(4)])


def on_device(queries, keys, values, span_order, doc_ids):
    bf16 = jnp.bfloat16
    me = lax.axis_index("tp").astype(jnp.int32)
    z = lax.axis_index("z").astype(jnp.int32)
    block = lax.axis_index(ALL[:-1]).astype(jnp.int32)
    me1, z1 = me.reshape(1), z.reshape(1)

    by_head = jnp.concatenate([keys.transpose(1, 0, 2), values.transpose(1, 0, 2)], axis=1)
    sent = by_head.reshape(4, 2, 16, 4, SPAN).transpose(2, 1, 0, 3, 4)
    sent = jnp.broadcast_to(sent[:, None], (16, 2, 2, 4, 4, SPAN)).reshape(256, 4, SPAN)
    sent, me1, z1, block = lax.optimization_barrier((sent, me1, z1, block))
    spread = lax.all_to_all(sent, ALL, 0, 0, tiled=True).reshape(128, 8, SPAN)

    pieces = pl.pallas_call(
        pieces_kernel,
        out_shape=[pltpu.VMEM((80, 8, SPAN), bf16)] * 4,
        in_specs=[SMEM, VMEM, VMEM],
        out_specs=[VMEM] * 4,
        compiler_params=pltpu.CompilerParams(vmem_limit_bytes=4 << 20),
        name="pieces",
    )(me1, queries.reshape(64, 4, 8, SPAN), by_head.reshape(4, 16, 8, SPAN))
    pieces = [pieces[0]] + [shifted(pieces[k], k) for k in range(1, 4)]

    windows = pl.pallas_call(
        windows_kernel,
        out_shape=pltpu.HBM((32, 2, BACK, 8, SPAN), bf16),
        in_specs=[SMEM, SMEM, VMEM],
        out_specs=ANY,
        scratch_shapes=[pltpu.VMEM((128 + BACK, 8, SPAN), bf16), pltpu.SemaphoreType.DMA((64,))],
        compiler_params=pltpu.CompilerParams(vmem_limit_bytes=4 << 20),
        name="windows",
    )(pltpu.with_memory_space_constraint(span_order, pltpu.HBM), z1, near(spread))
    windows = lax.all_to_all(windows.reshape(32, 256, SPAN), PLANE, 0, 0, tiled=True)

    doc_first = jnp.sum(
        (doc_ids[None, :] < jnp.arange(DOCS, dtype=jnp.int32)[:, None]).astype(jnp.int32), axis=1
    )
    spans = lax.dynamic_slice_in_dim(span_order, 2 * block, 2)
    docs = jnp.stack([lax.dynamic_slice_in_dim(doc_ids, spans[i] * SPAN, SPAN) for i in range(2)])
    start = jnp.sum(
        jnp.where(docs[:, :, None] == jnp.arange(DOCS, dtype=jnp.int32), doc_first, 0), axis=-1
    )
    first = start - (spans[:, None] - BACK) * SPAN
    reach = jnp.clip(BACK - first[:, 0] // SPAN, 0, BACK)
    first = jnp.broadcast_to(first.reshape(256, 1), (256, 8)).reshape(2048, 1)

    attended = pl.pallas_call(
        attention_kernel,
        out_shape=[pltpu.VMEM((64, 8, SPAN), bf16)] * 4,
        in_specs=[SMEM, SMEM] + [VMEM] * 6,
        out_specs=[VMEM] * 4,
        scratch_shapes=[pltpu.VMEM((4, 80, 8, SPAN), bf16), pltpu.VMEM((4, 64, 8, SPAN), bf16)],
        compiler_params=pltpu.CompilerParams(vmem_limit_bytes=24 << 20),
        name="attention",
    )(me1, reach, near(first), near(windows.reshape(32, 2, BACK, 8, SPAN)), *map(near, pieces))

    back = [attended[0]] + [shifted(attended[k], k) for k in range(1, 4)]
    result = pl.pallas_call(
        gather_kernel,
        out_shape=jax.ShapeDtypeStruct((64, 4, 8, SPAN), bf16),
        in_specs=[SMEM] + [VMEM] * 4,
        out_specs=VMEM,
        compiler_params=pltpu.CompilerParams(vmem_limit_bytes=4 << 20),
        name="gather",
    )(me1, *map(near, back))
    return result.reshape(64, 32, SPAN)


def solution(mesh):
    fine = Mesh(mesh.devices.reshape(4, 4, 2, 2, 4), ALL)
    placed = (P(ALL, None, None), P(ALL, None, None), P(ALL, None, None), P(), P())
    return jax.shard_map(
        on_device, mesh=fine, in_specs=placed, out_specs=P(ALL, None, None), check_vma=False
    )
```

```python
import math

import jax
import jax.numpy as jnp
from jax import lax
from jax.experimental import pallas as pl
from jax.experimental.pallas import tpu as pltpu
from jax.sharding import Mesh, PartitionSpec as P

SPAN = 128
HELD = 22
BACK = 16
DOCS = 32
ALL = ("y", "x", "z", "c", "tp")
PLANE = ("c", "y", "x")
NEG = -1e30


def pieces_kernel(me_ref, q_ref, kv_ref, p0, p1, p2, p3):
    me = me_ref[0]
    for k, out in enumerate((p0, p1, p2, p3)):
        head = lax.rem(me + k, 4)
        out[0:64] = q_ref[:, head]
        out[64:80] = kv_ref[head]


def windows_kernel(order_ref, z_ref, reach_ref, spread_ref, out_ref, ordered, lists, sems):
    z = z_ref[0]
    held = lists.shape[1]
    ordered[pl.ds(0, BACK)] = jnp.zeros((BACK, 8, SPAN), jnp.bfloat16)

    def place(slot, _):
        ordered[order_ref[slot] + BACK] = spread_ref[slot]
        return 0

    lax.fori_loop(0, 128, place, 0, unroll=8)

    def copy(dest):
        return pltpu.make_async_copy(lists.at[dest], out_ref.at[dest], sems.at[dest])

    def fill(dest, _):
        slot = 2 * (lax.rem(dest, 16) * 4 + z * 2 + dest // 16)
        first, second = order_ref[slot] + BACK - 1, order_ref[slot + 1] + BACK - held
        reach = reach_ref[slot]
        for at in range(BACK):
            if at < held - BACK:
                lists[dest, at] = ordered[first - at]
            else:
                lists[dest, at] = ordered[jnp.where(at < reach, first - at, second + at)]
        lists[dest, BACK:held] = ordered[pl.ds(second + BACK, held - BACK)]
        copy(dest).start()
        return 0

    lax.fori_loop(0, 32, fill, 0)

    def finish(dest, _):
        copy(dest).wait()
        return 0

    lax.fori_loop(0, 32, finish, 0)


def attention_kernel(me_ref, reach_ref, first_ref, kv_ref, p0, p1, p2, p3, o0, o1, o2, o3, own, out):
    me = me_ref[0]
    for k, piece in enumerate((p0, p1, p2, p3)):
        own[lax.rem(me + 4 - k, 4)] = piece[...]
    factor = math.log2(math.e) / math.sqrt(SPAN)

    held = kv_ref.shape[1]

    def slot_pass(slot, spans):
        rows = 512 if spans <= 8 else 256
        width = 16 * 8 * spans
        lane = lax.broadcasted_iota(jnp.int32, (1, width), 1)
        chunk, inner = lane // (8 * spans), lane % (8 * spans)
        span, r = inner // 8, inner % 8
        span = jnp.where(slot == 0, BACK - 1 - span, BACK - spans + span)
        rel = span * SPAN + (r // 4) * 64 + chunk * 4 + r % 4
        listed = pl.ds(slot * (held - spans), spans)
        keys = kv_ref[0:16, listed].reshape(width, SPAN)
        values = kv_ref[16:32, listed].reshape(width, SPAN)
        own_keys = jnp.concatenate([own[2 * slot + h, 64:72].reshape(64, SPAN) for h in range(2)], axis=0)
        own_values = jnp.concatenate([own[2 * slot + h, 72:80].reshape(64, SPAN) for h in range(2)], axis=0)
        own_rel = lax.broadcasted_iota(jnp.int32, (1, SPAN), 1) + BACK * SPAN
        for part in range(1024 // rows):
            half, at = part * rows // 512, part * rows % 512 // 8
            query = own[2 * slot + half, at : at + rows // 8].reshape(rows, SPAN)
            first = first_ref[pl.ds(slot * 1024 + part * rows, rows)]
            mine = (
                lax.broadcasted_iota(jnp.int32, (rows, 1), 0) // 8 + (part * rows // 8 + BACK * SPAN)
            )
            contract = (((1,), (1,)), ((), ()))
            far = lax.dot_general(query, keys, contract, preferred_element_type=jnp.float32)
            near = lax.dot_general(query, own_keys, contract, preferred_element_type=jnp.float32)
            far = jnp.where(rel >= first, far, NEG)
            near = jnp.where((own_rel >= first) & (own_rel <= mine), near, NEG)
            top = jnp.maximum(jnp.max(far, axis=1, keepdims=True), jnp.max(near, axis=1, keepdims=True))
            far = jnp.exp2((far - top) * factor)
            near = jnp.exp2((near - top) * factor)
            total = jnp.sum(far, axis=1, keepdims=True) + jnp.sum(near, axis=1, keepdims=True)
            summed = jnp.dot(far.astype(jnp.bfloat16), values, preferred_element_type=jnp.float32)
            summed += jnp.dot(near.astype(jnp.bfloat16), own_values, preferred_element_type=jnp.float32)
            to = lax.rem(2 * slot + half + 4 - me, 4)
            out[to, at : at + rows // 8] = (
                (summed / total).astype(jnp.bfloat16).reshape(rows // 8, 8, SPAN)
            )

    def one(slot, _):
        reach = reach_ref[slot]
        sizes = (2, 4, 8, BACK)
        for low, high in zip((-1,) + sizes[:-1], sizes):

            @pl.when((reach > low) & (reach <= high))
            def _(high=high):
                slot_pass(slot, high)

        return 0

    lax.fori_loop(0, 2, one, 0)

    for k, piece in enumerate((o0, o1, o2, o3)):
        piece[...] = out[k]


def gather_kernel(me_ref, r0, r1, r2, r3, out_ref):
    me = me_ref[0]
    for k, piece in enumerate((r0, r1, r2, r3)):
        out_ref[:, lax.rem(me + 4 - k, 4)] = piece[...]


SMEM = pl.BlockSpec(memory_space=pltpu.SMEM)
ANY = pl.BlockSpec(memory_space=pl.ANY)
VMEM = pl.BlockSpec(memory_space=pltpu.VMEM)


def near(array):
    return pltpu.with_memory_space_constraint(array, pltpu.VMEM)


def shifted(piece, by):
    return lax.ppermute(piece, "tp", [(i, (i + by) % 4) for i in range(4)])


def on_device(queries, keys, values, span_order, doc_ids):
    bf16 = jnp.bfloat16
    me = lax.axis_index("tp").astype(jnp.int32)
    z = lax.axis_index("z").astype(jnp.int32)
    block = lax.axis_index(ALL[:-1]).astype(jnp.int32)
    me1, z1 = me.reshape(1), z.reshape(1)

    by_head = jnp.concatenate([keys.transpose(1, 0, 2), values.transpose(1, 0, 2)], axis=1)
    sent = by_head.reshape(4, 2, 16, 4, SPAN).transpose(2, 1, 0, 3, 4)
    sent = jnp.broadcast_to(sent[:, None], (16, 2, 2, 4, 4, SPAN)).reshape(256, 4, SPAN)
    spread = lax.all_to_all(sent, ALL, 0, 0, tiled=True).reshape(128, 8, SPAN)

    pieces = pl.pallas_call(
        pieces_kernel,
        out_shape=[pltpu.VMEM((80, 8, SPAN), bf16)] * 4,
        in_specs=[SMEM, VMEM, VMEM],
        out_specs=[VMEM] * 4,
        compiler_params=pltpu.CompilerParams(vmem_limit_bytes=4 << 20),
        name="pieces",
    )(me1, queries.reshape(64, 4, 8, SPAN), by_head.reshape(4, 16, 8, SPAN))
    numbers = jnp.arange(DOCS, dtype=jnp.int32)
    doc_first = jnp.sum((doc_ids[None, :] < numbers[:, None]).astype(jnp.int32), axis=1)

    def start_of(docs):
        return jnp.sum(jnp.where(docs[..., None] == numbers, doc_first, 0), axis=-1)

    span_number = jnp.arange(128, dtype=jnp.int32)
    span_reach = span_number - start_of(doc_ids.reshape(128, SPAN)[:, 0]) // SPAN
    slot_reach = jnp.sum(jnp.where(span_order[:, None] == span_number, span_reach, 0), axis=-1)
    most = jnp.max(jnp.sum(slot_reach.reshape(64, 2), axis=1))

    spans = lax.dynamic_slice_in_dim(span_order, 2 * block, 2)
    docs = jnp.stack([lax.dynamic_slice_in_dim(doc_ids, spans[i] * SPAN, SPAN) for i in range(2)])
    first = start_of(docs) - (spans[:, None] - BACK) * SPAN
    reach = lax.dynamic_slice_in_dim(slot_reach, 2 * block, 2)
    first = jnp.broadcast_to(first.reshape(256, 1), (256, 8)).reshape(2048, 1)

    def path(held):
        def run(spread, slot_reach, span_order, me1, z1, reach, first, pieces):
            windows = pl.pallas_call(
                windows_kernel,
                out_shape=pltpu.HBM((32, held, 8, SPAN), bf16),
                in_specs=[SMEM, SMEM, SMEM, VMEM],
                out_specs=ANY,
                scratch_shapes=[
                    pltpu.VMEM((128 + BACK, 8, SPAN), bf16),
                    pltpu.VMEM((32, held, 8, SPAN), bf16),
                    pltpu.SemaphoreType.DMA((32,)),
                ],
                compiler_params=pltpu.CompilerParams(vmem_limit_bytes=6 << 20),
                name=f"windows_{held}",
            )(span_order, z1, slot_reach, near(spread))
            windows = lax.all_to_all(windows.reshape(32, held * 8, SPAN), PLANE, 0, 0, tiled=True)
            pieces = [pieces[0]] + [shifted(pieces[k], k) for k in range(1, 4)]
            attended = pl.pallas_call(
                attention_kernel,
                out_shape=[pltpu.VMEM((64, 8, SPAN), bf16)] * 4,
                in_specs=[SMEM, SMEM] + [VMEM] * 6,
                out_specs=[VMEM] * 4,
                scratch_shapes=[pltpu.VMEM((4, 80, 8, SPAN), bf16), pltpu.VMEM((4, 64, 8, SPAN), bf16)],
                compiler_params=pltpu.CompilerParams(vmem_limit_bytes=24 << 20),
                name=f"attention_{held}",
            )(me1, reach, near(first), near(windows.reshape(32, held, 8, SPAN)), *map(near, pieces))

            back = [attended[0]] + [shifted(attended[k], k) for k in range(1, 4)]
            return pl.pallas_call(
                gather_kernel,
                out_shape=pltpu.HBM((64, 4, 8, SPAN), bf16),
                in_specs=[SMEM] + [VMEM] * 4,
                out_specs=VMEM,
                compiler_params=pltpu.CompilerParams(vmem_limit_bytes=4 << 20),
                name="gather",
            )(me1, *map(near, back))

        return run

    result = lax.cond(
        most <= HELD, path(HELD), path(2 * BACK),
        spread, slot_reach, span_order, me1, z1, reach, first, tuple(pieces),
    )

    return result.reshape(64, 32, SPAN)


def solution(mesh):
    fine = Mesh(mesh.devices.reshape(4, 4, 2, 2, 4), ALL)
    placed = (P(ALL, None, None), P(ALL, None, None), P(ALL, None, None), P(), P())
    return jax.shard_map(
        on_device, mesh=fine, in_specs=placed, out_specs=P(ALL, None, None), check_vma=False
    )
```

```python
import math

import jax
import jax.numpy as jnp
from jax import lax
from jax.experimental import pallas as pl
from jax.experimental.pallas import tpu as pltpu
from jax.sharding import Mesh, PartitionSpec as P


SPAN = 128
HELD = 22
BACK = 16
DOCS = 32
ALL = ("y", "x", "z", "c", "tp")
PLANE = ("c", "y", "x")
NEG = -1e30


def pieces_kernel(me_ref, q_ref, kv_ref, p0, p1, p2, p3):
    me = me_ref[0]
    for k, out in enumerate((p0, p1, p2, p3)):
        head = lax.rem(me + k, 4)
        out[0:64] = q_ref[:, head]
        out[64:80] = kv_ref[head]


def reach_kernel(docs_ref, order_ref, reach_ref, most_ref):
    docs = docs_ref[...]
    row = lax.broadcasted_iota(jnp.int32, (128, 128), 0)
    lane = lax.broadcasted_iota(jnp.int32, (128, 128), 1)
    last = jnp.sum(jnp.where(row == lane, docs[:, 127:128], 0), axis=0, keepdims=True)
    same = (docs[:, 0:1] == last) & (lane < row)
    by_span = jnp.sum(same.astype(jnp.int32), axis=1, keepdims=True)
    by_slot = jnp.sum(jnp.where(row == order_ref[...], by_span, 0), axis=0, keepdims=True)
    reach_ref[...] = by_slot
    pairs = jnp.sum(jnp.where(row // 2 == lane // 2, by_slot, 0), axis=1, keepdims=True)
    most_ref[0] = jnp.max(pairs)


def windows_kernel(order_ref, z_ref, reach_ref, spread_ref, out_ref, ordered, lists, sems):
    z = z_ref[0]
    held = lists.shape[1]
    ordered[pl.ds(0, BACK)] = jnp.zeros((BACK, 8, SPAN), jnp.bfloat16)

    def place(slot, _):
        ordered[order_ref[slot] + BACK] = spread_ref[slot]
        return 0

    lax.fori_loop(0, 128, place, 0, unroll=8)

    def copy(dest):
        return pltpu.make_async_copy(lists.at[dest], out_ref.at[dest], sems.at[dest])

    def fill(dest, _):
        slot = 2 * (lax.rem(dest, 16) * 4 + z * 2 + dest // 16)
        first, second = order_ref[slot] + BACK - 1, order_ref[slot + 1] + BACK - held
        reach = reach_ref[slot]
        for at in range(BACK):
            if at < held - BACK:
                lists[dest, at] = ordered[first - at]
            else:
                lists[dest, at] = ordered[jnp.where(at < reach, first - at, second + at)]
        lists[dest, BACK:held] = ordered[pl.ds(second + BACK, held - BACK)]
        copy(dest).start()
        return 0

    lax.fori_loop(0, 32, fill, 0)

    def finish(dest, _):
        copy(dest).wait()
        return 0

    lax.fori_loop(0, 32, finish, 0)


def attention_kernel(me_ref, reach_ref, first_ref, kv_ref, p0, p1, p2, p3, o0, o1, o2, o3, own, out):
    me = me_ref[0]
    for k, piece in enumerate((p0, p1, p2, p3)):
        own[lax.rem(me + 4 - k, 4)] = piece[...]
    factor = math.log2(math.e) / math.sqrt(SPAN)

    held = kv_ref.shape[1]

    def slot_pass(slot, spans):
        rows = 512 if spans <= 8 else 256
        width = 16 * 8 * spans
        lane = lax.broadcasted_iota(jnp.int32, (1, width), 1)
        chunk, inner = lane // (8 * spans), lane % (8 * spans)
        span, r = inner // 8, inner % 8
        span = jnp.where(slot == 0, BACK - 1 - span, BACK - spans + span)
        rel = span * SPAN + (r // 4) * 64 + chunk * 4 + r % 4
        listed = pl.ds(slot * (held - spans), spans)
        keys = kv_ref[0:16, listed].reshape(width, SPAN)
        values = kv_ref[16:32, listed].reshape(width, SPAN)
        own_keys = jnp.concatenate([own[2 * slot + h, 64:72].reshape(64, SPAN) for h in range(2)], axis=0)
        own_values = jnp.concatenate([own[2 * slot + h, 72:80].reshape(64, SPAN) for h in range(2)], axis=0)
        own_rel = lax.broadcasted_iota(jnp.int32, (1, SPAN), 1) + BACK * SPAN
        for part in range(1024 // rows):
            half, at = part * rows // 512, part * rows % 512 // 8
            query = own[2 * slot + half, at : at + rows // 8].reshape(rows, SPAN)
            first = first_ref[pl.ds(slot * 1024 + part * rows, rows)]
            mine = (
                lax.broadcasted_iota(jnp.int32, (rows, 1), 0) // 8 + (part * rows // 8 + BACK * SPAN)
            )
            contract = (((1,), (1,)), ((), ()))
            far = lax.dot_general(query, keys, contract, preferred_element_type=jnp.float32)
            near = lax.dot_general(query, own_keys, contract, preferred_element_type=jnp.float32)
            far = jnp.where(rel >= first, far, NEG)
            near = jnp.where((own_rel >= first) & (own_rel <= mine), near, NEG)
            top = jnp.maximum(jnp.max(far, axis=1, keepdims=True), jnp.max(near, axis=1, keepdims=True))
            far = jnp.exp2((far - top) * factor)
            near = jnp.exp2((near - top) * factor)
            total = jnp.sum(far, axis=1, keepdims=True) + jnp.sum(near, axis=1, keepdims=True)
            summed = jnp.dot(far.astype(jnp.bfloat16), values, preferred_element_type=jnp.float32)
            summed += jnp.dot(near.astype(jnp.bfloat16), own_values, preferred_element_type=jnp.float32)
            to = lax.rem(2 * slot + half + 4 - me, 4)
            out[to, at : at + rows // 8] = (
                (summed / total).astype(jnp.bfloat16).reshape(rows // 8, 8, SPAN)
            )

    def one(slot, _):
        reach = reach_ref[slot]
        sizes = (2, 4, 8, BACK)
        for low, high in zip((-1,) + sizes[:-1], sizes):

            @pl.when((reach > low) & (reach <= high))
            def _(high=high):
                slot_pass(slot, high)

        return 0

    lax.fori_loop(0, 2, one, 0)

    for k, piece in enumerate((o0, o1, o2, o3)):
        piece[...] = out[k]


def gather_kernel(me_ref, r0, r1, r2, r3, out_ref):
    me = me_ref[0]
    for k, piece in enumerate((r0, r1, r2, r3)):
        out_ref[:, lax.rem(me + 4 - k, 4)] = piece[...]


SMEM = pl.BlockSpec(memory_space=pltpu.SMEM)
ANY = pl.BlockSpec(memory_space=pl.ANY)
VMEM = pl.BlockSpec(memory_space=pltpu.VMEM)


def near(array):
    return pltpu.with_memory_space_constraint(array, pltpu.VMEM)


def shifted(piece, by):
    return lax.ppermute(piece, "tp", [(i, (i + by) % 4) for i in range(4)])


def on_device(queries, keys, values, span_order, doc_ids):
    bf16 = jnp.bfloat16
    me = lax.axis_index("tp").astype(jnp.int32)
    z = lax.axis_index("z").astype(jnp.int32)
    block = lax.axis_index(ALL[:-1]).astype(jnp.int32)
    me1, z1 = me.reshape(1), z.reshape(1)

    slot_reach, most = pl.pallas_call(
        reach_kernel,
        out_shape=[jax.ShapeDtypeStruct((1, 128), jnp.int32), jax.ShapeDtypeStruct((1,), jnp.int32)],
        in_specs=[VMEM, VMEM],
        out_specs=[VMEM, SMEM],
        compiler_params=pltpu.CompilerParams(vmem_limit_bytes=4 << 20),
        name="reach",
    )(doc_ids.reshape(128, SPAN), span_order.reshape(1, 128))
    slot_reach = slot_reach.reshape(128)

    def path(held):
        def run(queries, keys, values, span_order, doc_ids, slot_reach):
            by_head = jnp.concatenate([keys.transpose(1, 0, 2), values.transpose(1, 0, 2)], axis=1)
            sent = by_head.reshape(4, 2, 16, 4, SPAN).transpose(2, 1, 0, 3, 4)
            sent = jnp.broadcast_to(sent[:, None], (16, 2, 2, 4, 4, SPAN)).reshape(256, 4, SPAN)
            spread = lax.all_to_all(sent, ALL, 0, 0, tiled=True)
            spread = spread.reshape(128, 8, SPAN)

            pieces = pl.pallas_call(
                pieces_kernel,
                out_shape=[pltpu.VMEM((80, 8, SPAN), bf16)] * 4,
                in_specs=[SMEM, VMEM, VMEM],
                out_specs=[VMEM] * 4,
                compiler_params=pltpu.CompilerParams(vmem_limit_bytes=4 << 20),
                name="pieces",
            )(me1, queries.reshape(64, 4, 8, SPAN), by_head.reshape(4, 16, 8, SPAN))
            pieces = [pieces[0]] + [shifted(pieces[k], k) for k in range(1, 4)]

            numbers = jnp.arange(DOCS, dtype=jnp.int32)
            doc_first = jnp.sum((doc_ids[None, :] < numbers[:, None]).astype(jnp.int32), axis=1)

            def start_of(docs):
                return jnp.sum(jnp.where(docs[..., None] == numbers, doc_first, 0), axis=-1)

            spans = lax.dynamic_slice_in_dim(span_order, 2 * block, 2)
            docs = jnp.stack([lax.dynamic_slice_in_dim(doc_ids, spans[i] * SPAN, SPAN) for i in range(2)])
            first = start_of(docs) - (spans[:, None] - BACK) * SPAN
            reach = lax.dynamic_slice_in_dim(slot_reach, 2 * block, 2)
            first = jnp.broadcast_to(first.reshape(256, 1), (256, 8)).reshape(2048, 1)

            windows = pl.pallas_call(
                windows_kernel,
                out_shape=pltpu.HBM((32, held, 8, SPAN), bf16),
                in_specs=[SMEM, SMEM, SMEM, VMEM],
                out_specs=ANY,
                scratch_shapes=[
                    pltpu.VMEM((128 + BACK, 8, SPAN), bf16),
                    pltpu.VMEM((32, held, 8, SPAN), bf16),
                    pltpu.SemaphoreType.DMA((32,)),
                ],
                compiler_params=pltpu.CompilerParams(vmem_limit_bytes=6 << 20),
            )(span_order, z1, slot_reach, near(spread))
            windows = lax.all_to_all(windows.reshape(32, held * 8, SPAN), PLANE, 0, 0, tiled=True)
            attended = pl.pallas_call(
                attention_kernel,
                out_shape=[pltpu.VMEM((64, 8, SPAN), bf16)] * 4,
                in_specs=[SMEM, SMEM] + [VMEM] * 6,
                out_specs=[VMEM] * 4,
                scratch_shapes=[pltpu.VMEM((4, 80, 8, SPAN), bf16), pltpu.VMEM((4, 64, 8, SPAN), bf16)],
                compiler_params=pltpu.CompilerParams(vmem_limit_bytes=24 << 20),
            )(me1, reach, near(first), near(windows.reshape(32, held, 8, SPAN)), *map(near, pieces))

            back = [attended[0]] + [shifted(attended[k], k) for k in range(1, 4)]
            return pl.pallas_call(
                gather_kernel,
                out_shape=pltpu.HBM((64, 4, 8, SPAN), bf16),
                in_specs=[SMEM] + [VMEM] * 4,
                out_specs=VMEM,
                compiler_params=pltpu.CompilerParams(vmem_limit_bytes=4 << 20),
                name="gather",
            )(me1, *map(near, back))

        return run

    result = lax.cond(
        most[0] <= HELD, path(HELD), path(2 * BACK),
        queries, keys, values, span_order, doc_ids, slot_reach,
    )
    return result.reshape(64, 32, SPAN)


def solution(mesh):
    fine = Mesh(mesh.devices.reshape(4, 4, 2, 2, 4), ALL)
    placed = (P(ALL, None, None), P(ALL, None, None), P(ALL, None, None), P(), P())
    return jax.shard_map(
        on_device, mesh=fine, in_specs=placed, out_specs=P(ALL, None, None), check_vma=False
    )
```

```python
import math

import jax
import jax.numpy as jnp
from jax import lax
from jax.experimental import pallas as pl
from jax.experimental.pallas import tpu as pltpu
from jax.sharding import Mesh, PartitionSpec as P

SPAN = 128
HELD = 24
BACK = 16
DOCS = 32
ALL = ("y", "x", "z", "c", "tp")
PLANE = ("c", "y", "x")
NEG = -1e30


def pieces_kernel(me_ref, q_ref, kv_ref, p0, p1, p2, p3):
    me = me_ref[0]
    for k, out in enumerate((p0, p1, p2, p3)):
        head = lax.rem(me + k, 4)
        out[0:64] = q_ref[:, head]
        out[64:80] = kv_ref[head]


def reach_kernel(docs_ref, order_ref, reach_ref, most_ref):
    docs = docs_ref[...]
    row = lax.broadcasted_iota(jnp.int32, (128, 128), 0)
    lane = lax.broadcasted_iota(jnp.int32, (128, 128), 1)
    last = jnp.sum(jnp.where(row == lane, docs[:, 127:128], 0), axis=0, keepdims=True)
    same = (docs[:, 0:1] == last) & (lane < row)
    by_span = jnp.sum(same.astype(jnp.int32), axis=1, keepdims=True)
    by_slot = jnp.sum(jnp.where(row == order_ref[...], by_span, 0), axis=0, keepdims=True)
    reach_ref[...] = by_slot
    pairs = jnp.sum(jnp.where(row // 2 == lane // 2, by_slot, 0), axis=1, keepdims=True)
    most_ref[0] = jnp.max(pairs)


def windows_kernel(order_ref, z_ref, reach_ref, spread_ref, out_ref, ordered, lists, sems):
    z = z_ref[0]
    held = lists.shape[1]
    ordered[pl.ds(0, BACK)] = jnp.zeros((BACK, 8, SPAN), jnp.bfloat16)

    def place(slot, _):
        ordered[order_ref[slot] + BACK] = spread_ref[slot]
        return 0

    lax.fori_loop(0, 128, place, 0, unroll=8)

    def copy(dest):
        return pltpu.make_async_copy(lists.at[dest], out_ref.at[dest], sems.at[dest])

    def fill(dest, _):
        slot = 2 * (lax.rem(dest, 16) * 4 + z * 2 + dest // 16)
        first, second = order_ref[slot] + BACK - 1, order_ref[slot + 1] + BACK - held
        reach = reach_ref[slot]
        for at in range(BACK):
            if at < held - BACK:
                lists[dest, at] = ordered[first - at]
            else:
                lists[dest, at] = ordered[jnp.where(at < reach, first - at, second + at)]
        lists[dest, BACK:held] = ordered[pl.ds(second + BACK, held - BACK)]
        copy(dest).start()
        return 0

    lax.fori_loop(0, 32, fill, 0)

    def finish(dest, _):
        copy(dest).wait()
        return 0

    lax.fori_loop(0, 32, finish, 0)


def attention_kernel(me_ref, reach_ref, first_ref, kv_ref, p0, p1, p2, p3, o0, o1, o2, o3, own, out):
    me = me_ref[0]
    for k, piece in enumerate((p0, p1, p2, p3)):
        own[lax.rem(me + 4 - k, 4)] = piece[...]
    factor = math.log2(math.e) / math.sqrt(SPAN)

    held = kv_ref.shape[1]

    def slot_pass(slot, spans):
        rows = 512 if spans <= 8 else 256
        width = 16 * 8 * spans
        lane = lax.broadcasted_iota(jnp.int32, (1, width), 1)
        chunk, inner = lane // (8 * spans), lane % (8 * spans)
        span, r = inner // 8, inner % 8
        span = jnp.where(slot == 0, BACK - 1 - span, BACK - spans + span)
        rel = span * SPAN + (r // 4) * 64 + chunk * 4 + r % 4
        listed = pl.ds(slot * (held - spans), spans)
        keys = kv_ref[0:16, listed].reshape(width, SPAN)
        values = kv_ref[16:32, listed].reshape(width, SPAN)
        own_keys = jnp.concatenate([own[2 * slot + h, 64:72].reshape(64, SPAN) for h in range(2)], axis=0)
        own_values = jnp.concatenate([own[2 * slot + h, 72:80].reshape(64, SPAN) for h in range(2)], axis=0)
        own_rel = lax.broadcasted_iota(jnp.int32, (1, SPAN), 1) + BACK * SPAN
        for part in range(1024 // rows):
            half, at = part * rows // 512, part * rows % 512 // 8
            query = own[2 * slot + half, at : at + rows // 8].reshape(rows, SPAN)
            first = first_ref[pl.ds(slot * 1024 + part * rows, rows)]
            mine = (
                lax.broadcasted_iota(jnp.int32, (rows, 1), 0) // 8 + (part * rows // 8 + BACK * SPAN)
            )
            contract = (((1,), (1,)), ((), ()))
            far = lax.dot_general(query, keys, contract, preferred_element_type=jnp.float32)
            near = lax.dot_general(query, own_keys, contract, preferred_element_type=jnp.float32)
            far = jnp.where(rel >= first, far, NEG)
            near = jnp.where((own_rel >= first) & (own_rel <= mine), near, NEG)
            top = jnp.maximum(jnp.max(far, axis=1, keepdims=True), jnp.max(near, axis=1, keepdims=True))
            far = jnp.exp2((far - top) * factor)
            near = jnp.exp2((near - top) * factor)
            total = jnp.sum(far, axis=1, keepdims=True) + jnp.sum(near, axis=1, keepdims=True)
            summed = jnp.dot(far.astype(jnp.bfloat16), values, preferred_element_type=jnp.float32)
            summed += jnp.dot(near.astype(jnp.bfloat16), own_values, preferred_element_type=jnp.float32)
            to = lax.rem(2 * slot + half + 4 - me, 4)
            out[to, at : at + rows // 8] = (
                (summed / total).astype(jnp.bfloat16).reshape(rows // 8, 8, SPAN)
            )

    def one(slot, _):
        reach = reach_ref[slot]
        sizes = (2, 4, 8, BACK)
        for low, high in zip((-1,) + sizes[:-1], sizes):

            @pl.when((reach > low) & (reach <= high))
            def _(high=high):
                slot_pass(slot, high)

        return 0

    lax.fori_loop(0, 2, one, 0)

    for k, piece in enumerate((o0, o1, o2, o3)):
        piece[...] = out[k]


def gather_kernel(me_ref, r0, r1, r2, r3, out_ref):
    me = me_ref[0]
    for k, piece in enumerate((r0, r1, r2, r3)):
        out_ref[:, lax.rem(me + 4 - k, 4)] = piece[...]


SMEM = pl.BlockSpec(memory_space=pltpu.SMEM)
ANY = pl.BlockSpec(memory_space=pl.ANY)
VMEM = pl.BlockSpec(memory_space=pltpu.VMEM)


def near(array):
    return pltpu.with_memory_space_constraint(array, pltpu.VMEM)


def shifted(piece, by):
    return lax.ppermute(piece, "tp", [(i, (i + by) % 4) for i in range(4)])


def on_device(queries, keys, values, span_order, doc_ids):
    bf16 = jnp.bfloat16
    me = lax.axis_index("tp").astype(jnp.int32)
    z = lax.axis_index("z").astype(jnp.int32)
    block = lax.axis_index(ALL[:-1]).astype(jnp.int32)
    me1, z1 = me.reshape(1), z.reshape(1)

    by_head = jnp.concatenate([keys.transpose(1, 0, 2), values.transpose(1, 0, 2)], axis=1)
    sent = by_head.reshape(4, 2, 16, 4, SPAN).transpose(2, 1, 0, 3, 4)
    sent = jnp.broadcast_to(sent[:, None], (16, 2, 2, 4, 4, SPAN)).reshape(256, 4, SPAN)
    spread = lax.all_to_all(sent, ALL, 0, 0, tiled=True).reshape(128, 8, SPAN)

    pieces = pl.pallas_call(
        pieces_kernel,
        out_shape=[pltpu.VMEM((80, 8, SPAN), bf16)] * 4,
        in_specs=[SMEM, VMEM, VMEM],
        out_specs=[VMEM] * 4,
        compiler_params=pltpu.CompilerParams(vmem_limit_bytes=4 << 20),
        name="pieces",
    )(me1, queries.reshape(64, 4, 8, SPAN), by_head.reshape(4, 16, 8, SPAN))
    slot_reach, most = pl.pallas_call(
        reach_kernel,
        out_shape=[jax.ShapeDtypeStruct((1, 128), jnp.int32), jax.ShapeDtypeStruct((1,), jnp.int32)],
        in_specs=[VMEM, VMEM],
        out_specs=[VMEM, SMEM],
        compiler_params=pltpu.CompilerParams(vmem_limit_bytes=4 << 20),
        name="reach",
    )(doc_ids.reshape(128, SPAN), span_order.reshape(1, 128))
    slot_reach = slot_reach.reshape(128)

    def path(held):
        def run(spread, slot_reach, span_order, doc_ids, pieces):
            numbers = jnp.arange(DOCS, dtype=jnp.int32)
            doc_first = jnp.sum((doc_ids[None, :] < numbers[:, None]).astype(jnp.int32), axis=1)

            def start_of(docs):
                return jnp.sum(jnp.where(docs[..., None] == numbers, doc_first, 0), axis=-1)

            spans = lax.dynamic_slice_in_dim(span_order, 2 * block, 2)
            docs = jnp.stack([lax.dynamic_slice_in_dim(doc_ids, spans[i] * SPAN, SPAN) for i in range(2)])
            first = start_of(docs) - (spans[:, None] - BACK) * SPAN
            reach = lax.dynamic_slice_in_dim(slot_reach, 2 * block, 2)
            first = jnp.broadcast_to(first.reshape(256, 1), (256, 8)).reshape(2048, 1)

            windows = pl.pallas_call(
                windows_kernel,
                out_shape=pltpu.HBM((32, held, 8, SPAN), bf16),
                in_specs=[SMEM, SMEM, SMEM, VMEM],
                out_specs=ANY,
                scratch_shapes=[
                    pltpu.VMEM((128 + BACK, 8, SPAN), bf16),
                    pltpu.VMEM((32, held, 8, SPAN), bf16),
                    pltpu.SemaphoreType.DMA((32,)),
                ],
                compiler_params=pltpu.CompilerParams(vmem_limit_bytes=6 << 20),
                name=f"windows_{held}",
            )(span_order, z1, slot_reach, near(spread))
            windows = lax.all_to_all(windows.reshape(32, held * 8, SPAN), PLANE, 0, 0, tiled=True)
            pieces = [pieces[0]] + [shifted(pieces[k], k) for k in range(1, 4)]
            attended = pl.pallas_call(
                attention_kernel,
                out_shape=[pltpu.VMEM((64, 8, SPAN), bf16)] * 4,
                in_specs=[SMEM, SMEM] + [VMEM] * 6,
                out_specs=[VMEM] * 4,
                scratch_shapes=[pltpu.VMEM((4, 80, 8, SPAN), bf16), pltpu.VMEM((4, 64, 8, SPAN), bf16)],
                compiler_params=pltpu.CompilerParams(vmem_limit_bytes=24 << 20),
                name=f"attention_{held}",
            )(me1, reach, near(first), near(windows.reshape(32, held, 8, SPAN)), *map(near, pieces))

            back = [attended[0]] + [shifted(attended[k], k) for k in range(1, 4)]
            return pl.pallas_call(
                gather_kernel,
                out_shape=pltpu.HBM((64, 4, 8, SPAN), bf16),
                in_specs=[SMEM] + [VMEM] * 4,
                out_specs=VMEM,
                compiler_params=pltpu.CompilerParams(vmem_limit_bytes=4 << 20),
                name="gather",
            )(me1, *map(near, back))

        return run

    result = lax.cond(
        most[0] <= HELD, path(HELD), path(2 * BACK),
        spread, slot_reach, span_order, doc_ids, tuple(pieces),
    )

    return result.reshape(64, 32, SPAN)


def solution(mesh):
    fine = Mesh(mesh.devices.reshape(4, 4, 2, 2, 4), ALL)
    placed = (P(ALL, None, None), P(ALL, None, None), P(ALL, None, None), P(), P())
    return jax.shard_map(
        on_device, mesh=fine, in_specs=placed, out_specs=P(ALL, None, None), check_vma=False
    )
```

```python
import math

import jax
import jax.numpy as jnp
from jax import lax
from jax.experimental import pallas as pl
from jax.experimental.pallas import tpu as pltpu
from jax.sharding import Mesh, PartitionSpec as P

SPAN = 128
HELD = 24
BACK = 16
DOCS = 32
ALL = ("y", "x", "z", "c", "tp")
PLANE = ("c", "y", "x")
NEG = -1e30


def spreading_kernel(keys_ref, values_ref, sent_ref):
    for core, ref in enumerate((keys_ref, values_ref)):
        by_head = jnp.swapaxes(ref[...].reshape(16, 4, 4, SPAN), 1, 2)
        for plane in range(2):
            sent_ref[:, plane, core] = by_head


def pieces_kernel(me_ref, q_ref, kv_ref, p0, p1, p2, p3):
    me = me_ref[0]
    for k, out in enumerate((p0, p1, p2, p3)):
        head = lax.rem(me + k, 4)
        out[0:64] = q_ref[:, head]
        out[64:80] = kv_ref[head]


def reach_kernel(docs_ref, order_ref, reach_ref, most_ref):
    docs = docs_ref[...]
    row = lax.broadcasted_iota(jnp.int32, (128, 128), 0)
    lane = lax.broadcasted_iota(jnp.int32, (128, 128), 1)
    last = jnp.sum(jnp.where(row == lane, docs[:, 127:128], 0), axis=0, keepdims=True)
    same = (docs[:, 0:1] == last) & (lane < row)
    by_span = jnp.sum(same.astype(jnp.int32), axis=1, keepdims=True)
    by_slot = jnp.sum(jnp.where(row == order_ref[...], by_span, 0), axis=0, keepdims=True)
    reach_ref[...] = by_slot
    pairs = jnp.sum(jnp.where(row // 2 == lane // 2, by_slot, 0), axis=1, keepdims=True)
    most_ref[0] = jnp.max(pairs)


def windows_kernel(order_ref, z_ref, reach_ref, spread_ref, out_ref, ordered, lists, sems):
    z = z_ref[0]
    held = lists.shape[1]
    ordered[pl.ds(0, BACK)] = jnp.zeros((BACK, 8, SPAN), jnp.bfloat16)

    def place(slot, _):
        ordered[order_ref[slot] + BACK] = spread_ref[slot]
        return 0

    lax.fori_loop(0, 128, place, 0, unroll=16)

    def copy(dest):
        return pltpu.make_async_copy(lists.at[dest], out_ref.at[dest], sems.at[dest])

    def fill(dest, _):
        slot = 2 * (lax.rem(dest, 16) * 4 + z * 2 + dest // 16)
        first, second = order_ref[slot] + BACK - 1, order_ref[slot + 1] + BACK - held
        reach = reach_ref[slot]
        for at in range(BACK):
            if at < held - BACK:
                lists[dest, at] = ordered[first - at]
            else:
                lists[dest, at] = ordered[jnp.where(at < reach, first - at, second + at)]
        lists[dest, BACK:held] = ordered[pl.ds(second + BACK, held - BACK)]
        copy(dest).start()
        return 0

    lax.fori_loop(0, 32, fill, 0, unroll=4)

    def finish(dest, _):
        copy(dest).wait()
        return 0

    lax.fori_loop(0, 32, finish, 0, unroll=8)


def attention_kernel(me_ref, reach_ref, first_ref, kv_ref, p0, p1, p2, p3, o0, o1, o2, o3, own, out):
    me = me_ref[0]
    for k, piece in enumerate((p0, p1, p2, p3)):
        own[lax.rem(me + 4 - k, 4)] = piece[...]
    factor = math.log2(math.e) / math.sqrt(SPAN)

    held = kv_ref.shape[1]

    def slot_pass(slot, spans):
        rows = 512 if spans <= 8 else 256
        width = 16 * 8 * spans
        lane = lax.broadcasted_iota(jnp.int32, (1, width), 1)
        chunk, inner = lane // (8 * spans), lane % (8 * spans)
        span, r = inner // 8, inner % 8
        span = jnp.where(slot == 0, BACK - 1 - span, BACK - spans + span)
        rel = span * SPAN + (r // 4) * 64 + chunk * 4 + r % 4
        listed = pl.ds(slot * (held - spans), spans)
        keys = kv_ref[0:16, listed].reshape(width, SPAN)
        values = kv_ref[16:32, listed].reshape(width, SPAN)
        own_keys = jnp.concatenate([own[2 * slot + h, 64:72].reshape(64, SPAN) for h in range(2)], axis=0)
        own_values = jnp.concatenate([own[2 * slot + h, 72:80].reshape(64, SPAN) for h in range(2)], axis=0)
        own_rel = lax.broadcasted_iota(jnp.int32, (1, SPAN), 1) + BACK * SPAN
        for part in range(1024 // rows):
            half, at = part * rows // 512, part * rows % 512 // 8
            query = own[2 * slot + half, at : at + rows // 8].reshape(rows, SPAN)
            first = first_ref[pl.ds(slot * 1024 + part * rows, rows)]
            mine = (
                lax.broadcasted_iota(jnp.int32, (rows, 1), 0) // 8 + (part * rows // 8 + BACK * SPAN)
            )
            contract = (((1,), (1,)), ((), ()))
            far = lax.dot_general(query, keys, contract, preferred_element_type=jnp.float32)
            near = lax.dot_general(query, own_keys, contract, preferred_element_type=jnp.float32)
            far = jnp.where(rel >= first, far, NEG)
            near = jnp.where((own_rel >= first) & (own_rel <= mine), near, NEG)
            top = jnp.maximum(jnp.max(far, axis=1, keepdims=True), jnp.max(near, axis=1, keepdims=True))
            far = jnp.exp2((far - top) * factor)
            near = jnp.exp2((near - top) * factor)
            total = jnp.sum(far, axis=1, keepdims=True) + jnp.sum(near, axis=1, keepdims=True)
            summed = jnp.dot(far.astype(jnp.bfloat16), values, preferred_element_type=jnp.float32)
            summed += jnp.dot(near.astype(jnp.bfloat16), own_values, preferred_element_type=jnp.float32)
            to = lax.rem(2 * slot + half + 4 - me, 4)
            out[to, at : at + rows // 8] = (
                (summed / total).astype(jnp.bfloat16).reshape(rows // 8, 8, SPAN)
            )

    def one(slot, _):
        reach = reach_ref[slot]
        sizes = (2, 4, 8, BACK)
        for low, high in zip((-1,) + sizes[:-1], sizes):

            @pl.when((reach > low) & (reach <= high))
            def _(high=high):
                slot_pass(slot, high)

        return 0

    lax.fori_loop(0, 2, one, 0)

    for k, piece in enumerate((o0, o1, o2, o3)):
        piece[...] = out[k]


def gather_kernel(me_ref, r0, r1, r2, r3, out_ref):
    me = me_ref[0]
    for k, piece in enumerate((r0, r1, r2, r3)):
        out_ref[:, lax.rem(me + 4 - k, 4)] = piece[...]


SMEM = pl.BlockSpec(memory_space=pltpu.SMEM)
ANY = pl.BlockSpec(memory_space=pl.ANY)
VMEM = pl.BlockSpec(memory_space=pltpu.VMEM)


def far(array):
    return pltpu.with_memory_space_constraint(array, pltpu.HBM)


def near(array):
    return pltpu.with_memory_space_constraint(array, pltpu.VMEM)


def shifted(piece, by):
    return lax.ppermute(piece, "tp", [(i, (i + by) % 4) for i in range(4)])


def on_device(queries, keys, values, span_order, doc_ids):
    bf16 = jnp.bfloat16
    me = lax.axis_index("tp").astype(jnp.int32)
    z = lax.axis_index("z").astype(jnp.int32)
    block = lax.axis_index(ALL[:-1]).astype(jnp.int32)
    me1, z1 = me.reshape(1), z.reshape(1)

    by_head = jnp.concatenate([keys.transpose(1, 0, 2), values.transpose(1, 0, 2)], axis=1)
    sent = pl.pallas_call(
        spreading_kernel,
        out_shape=pltpu.HBM((16, 2, 2, 4, 4, SPAN), bf16),
        in_specs=[VMEM, VMEM],
        out_specs=VMEM,
        compiler_params=pltpu.CompilerParams(vmem_limit_bytes=4 << 20),
        name="spreading",
    )(far(keys), far(values)).reshape(256, 4, SPAN)
    spread = lax.all_to_all(sent, ALL, 0, 0, tiled=True).reshape(128, 8, SPAN)

    pieces = pl.pallas_call(
        pieces_kernel,
        out_shape=[pltpu.HBM((80, 8, SPAN), bf16)] * 4,
        in_specs=[SMEM, VMEM, VMEM],
        out_specs=[VMEM] * 4,
        compiler_params=pltpu.CompilerParams(vmem_limit_bytes=4 << 20),
        name="pieces",
    )(me1, queries.reshape(64, 4, 8, SPAN), by_head.reshape(4, 16, 8, SPAN))
    slot_reach, most = pl.pallas_call(
        reach_kernel,
        out_shape=[jax.ShapeDtypeStruct((1, 128), jnp.int32), jax.ShapeDtypeStruct((1,), jnp.int32)],
        in_specs=[VMEM, VMEM],
        out_specs=[VMEM, SMEM],
        compiler_params=pltpu.CompilerParams(vmem_limit_bytes=4 << 20),
        name="reach",
    )(doc_ids.reshape(128, SPAN), span_order.reshape(1, 128))
    slot_reach = slot_reach.reshape(128)

    def path(held):
        def run(spread, slot_reach, span_order, doc_ids, pieces):
            numbers = jnp.arange(DOCS, dtype=jnp.int32)
            doc_first = jnp.sum((doc_ids[None, :] < numbers[:, None]).astype(jnp.int32), axis=1)

            def start_of(docs):
                return jnp.sum(jnp.where(docs[..., None] == numbers, doc_first, 0), axis=-1)

            spans = lax.dynamic_slice_in_dim(span_order, 2 * block, 2)
            docs = jnp.stack([lax.dynamic_slice_in_dim(doc_ids, spans[i] * SPAN, SPAN) for i in range(2)])
            first = start_of(docs) - (spans[:, None] - BACK) * SPAN
            reach = lax.dynamic_slice_in_dim(slot_reach, 2 * block, 2)
            first = jnp.broadcast_to(first.reshape(256, 1), (256, 8)).reshape(2048, 1)

            windows = pl.pallas_call(
                windows_kernel,
                out_shape=pltpu.HBM((32, held, 8, SPAN), bf16),
                in_specs=[SMEM, SMEM, SMEM, VMEM],
                out_specs=ANY,
                scratch_shapes=[
                    pltpu.VMEM((128 + BACK, 8, SPAN), bf16),
                    pltpu.VMEM((32, held, 8, SPAN), bf16),
                    pltpu.SemaphoreType.DMA((32,)),
                ],
                compiler_params=pltpu.CompilerParams(vmem_limit_bytes=6 << 20),
                name=f"windows_{held}",
            )(span_order, z1, slot_reach, near(spread))
            windows = lax.all_to_all(windows.reshape(32, held * 8, SPAN), PLANE, 0, 0, tiled=True)
            pieces = [pieces[0]] + [shifted(pieces[k], k) for k in range(1, 4)]
            attended = pl.pallas_call(
                attention_kernel,
                out_shape=[pltpu.VMEM((64, 8, SPAN), bf16)] * 4,
                in_specs=[SMEM, SMEM] + [VMEM] * 6,
                out_specs=[VMEM] * 4,
                scratch_shapes=[pltpu.VMEM((4, 80, 8, SPAN), bf16), pltpu.VMEM((4, 64, 8, SPAN), bf16)],
                compiler_params=pltpu.CompilerParams(vmem_limit_bytes=24 << 20),
                name=f"attention_{held}",
            )(me1, reach, near(first), near(windows.reshape(32, held, 8, SPAN)), *map(near, pieces))

            back = [attended[0]] + [shifted(attended[k], k) for k in range(1, 4)]
            return pl.pallas_call(
                gather_kernel,
                out_shape=pltpu.HBM((64, 4, 8, SPAN), bf16),
                in_specs=[SMEM] + [VMEM] * 4,
                out_specs=VMEM,
                compiler_params=pltpu.CompilerParams(vmem_limit_bytes=4 << 20),
                name="gather",
            )(me1, *map(near, back))

        return run

    result = lax.cond(
        most[0] <= HELD, path(HELD), path(2 * BACK),
        spread, slot_reach, span_order, doc_ids, tuple(pieces),
    )

    return result.reshape(64, 32, SPAN)


def solution(mesh):
    fine = Mesh(mesh.devices.reshape(4, 4, 2, 2, 4), ALL)
    placed = (P(ALL, None, None), P(ALL, None, None), P(ALL, None, None), P(), P())
    return jax.shard_map(
        on_device, mesh=fine, in_specs=placed, out_specs=P(ALL, None, None), check_vma=False
    )
```
